256 devices in a mesh: seq: 64 (over z, y, core), tp: 4 (over x).
Axes of the slice: x: 4, y: 4, z: 8, core: 2. Of those that a mesh axis runs over, the one named last changes fastest.
Arguments:
- q_new: bfloat16 [32768, 8192], P('seq', 'tp'), may hold values from -16 to 16
- k_new: bfloat16 [32768, 1024], P('seq', 'tp'), may hold values from -6 to 6
- v_new: bfloat16 [32768, 1024], P('seq', 'tp'), may hold values from -6 to 6
- q_bias: bfloat16 [8192], P('tp'), may hold values from -3 to 3
- k_bias: bfloat16 [1024], P('tp'), may hold values from -3 to 3
- v_bias: bfloat16 [1024], P('tp'), may hold values from -3 to 3
- cache_k: bfloat16 [131072, 1024], P('seq', 'tp'), may hold values from -16 to 16
- cache_v: bfloat16 [131072, 1024], P('seq', 'tp'), may hold values from -6 to 6
- deal: int32 [64], replicated, may hold values from 0 to 63, each once
- cache_len: int32 [64], replicated, may hold values from 1 to 2048, 65536 in all
Outputs:
- attn_out: bfloat16 [32768, 8192], P('seq', 'tp')
- new_keys: bfloat16 [32768, 1024], P('seq', 'tp')
- new_values: bfloat16 [32768, 1024], P('seq', 'tp')
- last_norm: float32 [64], P('seq')
- top_logit: float32 [64], P('seq')
The draws below stay inside these ranges and needn't reach their ends.
Inputs may be any that keep to these rules, and one draw needn't show every extreme that they name: `deal`: each request fills exactly one slot. `cache_len`: the lengths sum to 65536 and the largest is exactly 2048.
All inputs are finite; a program needn't handle non-finite values.
Results may differ from the reference program's by a relative error of at most 0.012.
Values may be sent and summed in bfloat16 or wider, within the bound.
A program may use at most 192 MiB of HBM per device.

```python
import math
import jax
import jax.numpy as jnp
import numpy as np
from jax import lax

HQ = 64
KVH = 8
HEAD = 128
NEW = 512
CACHE = 2048
REQUESTS = 64
TOKENS = 32768
CACHE_ROWS = 131072


def lifted_rows(key, shape):
    return jnp.clip(jax.random.normal(key, shape, jnp.float32), -4.0, 4.0)


def draw_q_new(key, part):
    return lifted_rows(jax.random.fold_in(key, 11), (TOKENS, HQ * HEAD)).astype(jnp.bfloat16)


def draw_cache_k(key, part):
    return lifted_rows(jax.random.fold_in(key, 23), (CACHE_ROWS, KVH * HEAD)).astype(jnp.bfloat16)


def steps_of(own_key, extent, pieces, low, high):
    gain, own = 1.0, jax.random.fold_in(own_key, 6)
    for axis_at, parts in pieces:
        heights = jnp.exp(jax.random.uniform(jax.random.fold_in(own, axis_at), (parts,), jnp.float32, low / len(pieces), high / len(pieces)))
        gain = gain * jnp.repeat(heights, extent[axis_at] // parts).reshape([-1 if axis == axis_at else 1 for axis in range(len(extent))])
    return gain


def profile(amount, total, bound, lean):
    loads = [(1 << 20) // math.isqrt(grade ** lean) + 1 for grade in range(2, amount + 1)]
    rest, counts = total - bound - (amount - 1), [1] * (amount - 1)
    while rest > 0:
        movable = [i for i in range(amount - 1) if counts[i] < bound]
        whole, left = sum([loads[i] for i in movable]), rest
        for i in movable:
            extra = min(bound - counts[i], max(1, left * loads[i] // whole), rest)
            counts[i] = counts[i] + extra
            rest = rest - extra
    return np.array([bound] + counts)


def ragged_sizes(own_key, amount, total, most, skew):
    if amount == 2:
        one = jax.random.randint(own_key, (), max(1, total - most), min(most, total - 1) + 1)
        return jnp.stack([one, total - one])
    tallies = jnp.asarray(profile(amount, total, most, skew), jnp.int32)
    couples = (amount - 1) // 2
    donor, receiver = tallies[1:1 + 2 * couples:2], tallies[2:2 + 2 * couples:2]
    room = jnp.minimum(donor - 1, most - receiver)
    shifted = jax.random.randint(jax.random.fold_in(own_key, 1), (couples,), 0, 1 << 20) % (room + 1)
    tallies = tallies.at[1:1 + 2 * couples:2].set(donor - shifted).at[2:2 + 2 * couples:2].set(receiver + shifted)
    return tallies[jax.random.permutation(jax.random.fold_in(own_key, 2), amount)]


def bell_draw(own_key, dims, width, limit, cuts=(), kind=jnp.bfloat16):
    entries = width * jax.random.normal(own_key, dims, jnp.float32)
    if cuts:
        entries = entries * steps_of(own_key, dims, cuts, -0.22, 0.18)
    return jnp.clip(entries, -limit, limit).astype(kind)


def setup_inputs(seed: int = 0) -> dict:
    seeds = jax.random.split(jax.random.key(seed), 11)
    q_new = draw_q_new(jax.random.fold_in(seeds[10], 71), 0)
    k_new = bell_draw(seeds[1], (TOKENS, KVH * HEAD), 1.0, 6.0, ((0, 64), (1, 4)))
    v_new = bell_draw(seeds[2], (TOKENS, KVH * HEAD), 1.0, 6.0, ((0, 64), (1, 4)))
    q_bias = bell_draw(seeds[3], (HQ * HEAD,), 0.5, 3.0, ((0, 4),))
    k_bias = bell_draw(seeds[4], (KVH * HEAD,), 0.5, 3.0, ((0, 4),))
    v_bias = bell_draw(seeds[5], (KVH * HEAD,), 0.5, 3.0, ((0, 4),))
    cache_k = draw_cache_k(jax.random.fold_in(seeds[10], 71), 0)
    cache_v = bell_draw(seeds[7], (CACHE_ROWS, KVH * HEAD), 1.0, 6.0, ((0, 64), (1, 4)))
    deal = jax.random.permutation(seeds[8], REQUESTS).astype(jnp.int32)
    cache_len = ragged_sizes(seeds[9], REQUESTS, REQUESTS * CACHE // 2, CACHE, 2).astype(jnp.int32)
    return {"q_new": q_new, "k_new": k_new, "v_new": v_new, "q_bias": q_bias, "k_bias": k_bias, "v_bias": v_bias, "cache_k": cache_k, "cache_v": cache_v, "deal": deal, "cache_len": cache_len}


theta_base = 1000000.0

def rotate(vectors, positions):
    half_dim = vectors.shape[-1] // 2
    frequency = theta_base ** (-2.0 * jnp.arange(half_dim, dtype=jnp.float32) / vectors.shape[-1])
    angles = positions.astype(jnp.float32)[:, None] * frequency[None, :]
    cosine = jnp.cos(angles)[:, None, :]
    sine_part = jnp.sin(angles)[:, None, :]
    lower_part = vectors[..., :half_dim]
    upper_part = vectors[..., half_dim:]
    return jnp.concatenate([lower_part * cosine - upper_part * sine_part, upper_part * cosine + lower_part * sine_part], axis=-1)

def reference(q_new, k_new, v_new, q_bias, k_bias, v_bias, cache_k, cache_v, deal, cache_len):
    group = HQ // KVH
    slot_ids = jnp.arange(REQUESTS, dtype=jnp.int32)
    inverse = lax.optimization_barrier(jnp.sum(jnp.where(deal[None, :] == slot_ids[:, None], slot_ids[None, :], 0), axis=1)).astype(jnp.int32)
    q_req = jnp.take(q_new.reshape(REQUESTS, NEW, HQ * HEAD), inverse, axis=0)
    k_req = jnp.take(k_new.reshape(REQUESTS, NEW, KVH * HEAD), inverse, axis=0)
    v_req = jnp.take(v_new.reshape(REQUESTS, NEW, KVH * HEAD), inverse, axis=0)

    def one_request(item):
        q_raw, k_raw, v_raw, stored_k, stored_v, length = item
        positions = length + jnp.arange(NEW, dtype=jnp.int32)
        queries = rotate((q_raw.astype(jnp.float32) + q_bias.astype(jnp.float32)).reshape(NEW, HQ, HEAD), positions).astype(jnp.bfloat16)
        fresh_keys = rotate((k_raw.astype(jnp.float32) + k_bias.astype(jnp.float32)).reshape(NEW, KVH, HEAD), positions).astype(jnp.bfloat16)
        fresh_values = (v_raw.astype(jnp.float32) + v_bias.astype(jnp.float32)).astype(jnp.bfloat16).reshape(NEW, KVH, HEAD)
        key_rows = jnp.concatenate([stored_k.reshape(CACHE, KVH, HEAD), fresh_keys], axis=0).astype(jnp.float32)
        value_rows = jnp.concatenate([stored_v.reshape(CACHE, KVH, HEAD), fresh_values], axis=0).astype(jnp.float32)
        grouped = queries.reshape(NEW, KVH, group, HEAD).astype(jnp.float32)
        scores = jnp.einsum('qkgd,tkd->kgqt', grouped, key_rows) * HEAD ** (-0.5)
        row_ids = jnp.arange(NEW, dtype=jnp.int32)[:, None]
        col_ids = jnp.arange(CACHE + NEW, dtype=jnp.int32)[None, :]
        valid = (col_ids < length) | (col_ids >= CACHE) & (col_ids - CACHE <= row_ids)
        scores = jnp.where(valid, scores, -jnp.inf)
        running_max = lax.optimization_barrier(jnp.max(scores, axis=-1))
        weight = jnp.exp(scores - running_max[..., None])
        row_total = lax.optimization_barrier(jnp.sum(weight, axis=-1))
        rounded = lax.optimization_barrier(weight.astype(jnp.bfloat16)).astype(jnp.float32)
        weighted = jnp.einsum('kgqt,tkd->kgqd', rounded, value_rows)
        mixture = (weighted / row_total[..., None]).transpose(2, 0, 1, 3).reshape(NEW, HQ * HEAD)
        last_row = mixture[NEW - 1]
        norm_value = jnp.sqrt(jnp.mean(last_row * last_row) + 1e-06)
        top_value = jnp.max(running_max[:, :, NEW - 1])
        return (mixture.astype(jnp.bfloat16), fresh_keys.reshape(NEW, KVH * HEAD), fresh_values.reshape(NEW, KVH * HEAD), norm_value, top_value)
    results = lax.map(one_request, (q_req, k_req, v_req, cache_k.reshape(REQUESTS, CACHE, KVH * HEAD), cache_v.reshape(REQUESTS, CACHE, KVH * HEAD), cache_len))
    return (results[0].reshape(TOKENS, HQ * HEAD), results[1].reshape(TOKENS, KVH * HEAD), results[2].reshape(TOKENS, KVH * HEAD), results[3], results[4])
```

```python
import functools
import math

import jax
import jax.numpy as jnp
from jax import lax
from jax.experimental import pallas as pl
from jax.experimental.pallas import tpu as pltpu
from jax.sharding import PartitionSpec as P

HEAD = 128
MESH = pl.DeviceIdType.MESH

theta_base = 1000000.0
norm_epsilon = 1e-06
scale = HEAD**-0.5
exp2_scale = scale * math.log2(math.e)
low_score = -3.0e38


def tables(length, rows):
    half_dim = HEAD // 2
    positions = length + jnp.arange(rows, dtype=jnp.int32)
    frequency = theta_base ** (-2.0 * jnp.arange(half_dim, dtype=jnp.float32) / HEAD)
    angles = positions.astype(jnp.float32)[:, None] * frequency[None, :]
    cosine, sine = jnp.cos(angles), jnp.sin(angles)
    return (
        jnp.concatenate([cosine, cosine], axis=1),
        jnp.concatenate([-sine, sine], axis=1),
    )


def rope(x, cosine, sine):
    return x * cosine + pltpu.roll(x, HEAD // 2, 1) * sine


def attention_kernel(
    length_ref, tok, q_bias, k_bias, v_bias, cache_k, cache_v, cosine, sine,
    out, new_keys, new_values, stats,
    keys, values, s_a, s_b, m_a, m_b,
):
    rows = tok.shape[1]
    kv_count = tok.shape[0]
    cached = cache_k.shape[0]
    group = tok.shape[2] // HEAD - 2
    half = 256
    halves = rows // half
    length = length_ref[0]

    stats[...] = jnp.zeros_like(stats)
    stats[1:2, :] = jnp.full((1, HEAD), low_score, jnp.float32)
    causal = lax.broadcasted_iota(jnp.int32, (half, half), 1) <= lax.broadcasted_iota(
        jnp.int32, (half, half), 0
    )

    def prepare(kv):
        at = slice(kv * HEAD, (kv + 1) * HEAD)
        valid = lax.broadcasted_iota(jnp.int32, (cached, HEAD), 0) < length
        keys[:cached, :] = jnp.where(valid, cache_k[:, at], cache_k[0:1, at])
        values[:cached, :HEAD] = jnp.where(valid, cache_v[:, at], jnp.bfloat16(0))
        values[:cached, HEAD:] = jnp.where(valid, jnp.bfloat16(1), jnp.bfloat16(0))
        fresh = tok[kv, :, group * HEAD : (group + 1) * HEAD].astype(jnp.float32)
        fresh = fresh + k_bias[0:1, at].astype(jnp.float32)
        fresh = rope(fresh, cosine[...], sine[...]).astype(jnp.bfloat16)
        keys[cached:, :] = fresh
        new_keys[:, at] = fresh
        fresh = tok[kv, :, (group + 1) * HEAD :].astype(jnp.float32)
        fresh = (fresh + v_bias[0:1, at].astype(jnp.float32)).astype(jnp.bfloat16)
        values[cached:, :HEAD] = fresh
        values[cached:, HEAD:] = jnp.ones((rows, HEAD), jnp.bfloat16)
        new_values[:, at] = fresh

    def key_blocks(part):
        blocks = [(first, False) for first in range(0, cached, half)]
        blocks += [(cached + half * i, i == part) for i in range(part + 1)]
        return blocks

    def score(kv, head, s_ref, m_ref):
        at = pl.ds(pl.multiple_of(head * HEAD, HEAD), HEAD)
        bias_at = pl.ds(pl.multiple_of((kv * group + head) * HEAD, HEAD), HEAD)
        bias = q_bias[0:1, bias_at].astype(jnp.float32)
        for part in range(halves):
            here = slice(part * half, (part + 1) * half)
            x = tok[kv, here, at].astype(jnp.float32) + bias
            query = rope(x, cosine[here, :], sine[here, :]).astype(jnp.bfloat16)
            largest = None
            for first, masked in key_blocks(part):
                s = lax.dot_general(
                    query, keys[first : first + half, :],
                    (((1,), (1,)), ((), ())), preferred_element_type=jnp.float32,
                )
                if masked:
                    s = jnp.where(causal, s, low_score)
                s_ref[here, first : first + half] = s
                local = jnp.maximum(s[:, :HEAD], s[:, HEAD:])
                largest = local if largest is None else jnp.maximum(largest, local)
            m_ref[here, :] = jnp.broadcast_to(
                jnp.max(largest, axis=1, keepdims=True), (half, HEAD)
            )

    def mix(kv, head, s_ref, m_ref):
        out_at = pl.ds(pl.multiple_of((kv * group + head) * HEAD, HEAD), HEAD)
        for part in range(halves):
            here = slice(part * half, (part + 1) * half)
            m = m_ref[here, :]
            m2 = jnp.concatenate([m, m], axis=1)
            total = None
            for first, masked in key_blocks(part):
                w = jnp.exp2((s_ref[here, first : first + half] - m2) * exp2_scale)
                term = jnp.dot(
                    w.astype(jnp.bfloat16), values[first : first + half, :],
                    preferred_element_type=jnp.float32,
                )
                total = term if total is None else total + term
            mixture = total[:, :HEAD] / total[:, HEAD:]
            out[here, out_at] = mixture.astype(jnp.bfloat16)
            if part == halves - 1:
                last = mixture[half - 1 : half, :]
                stats[0:1, :] = stats[0:1, :] + last * last
                stats[1:2, :] = jnp.maximum(stats[1:2, :], m[half - 1 : half, :] * scale)

    for kv in range(kv_count):
        prepare(kv)
        score(kv, 0, s_a, m_a)

        @pl.loop(0, group // 2 - 1)
        def _(i):
            score(kv, 2 * i + 1, s_b, m_b)
            mix(kv, 2 * i, s_a, m_a)
            score(kv, 2 * i + 2, s_a, m_a)
            mix(kv, 2 * i + 1, s_b, m_b)

        score(kv, group - 1, s_b, m_b)
        mix(kv, group - 2, s_a, m_a)
        mix(kv, group - 1, s_b, m_b)


def attend(length, tok, q_bias, k_bias, v_bias, cache_k, cache_v, cosine, sine):
    kv_count, rows, _ = tok.shape
    cached = cache_k.shape[0]
    vmem = pl.BlockSpec(memory_space=pltpu.VMEM)
    return pl.pallas_call(
        attention_kernel,
        out_shape=(
            jax.ShapeDtypeStruct((rows, q_bias.shape[0]), jnp.bfloat16),
            jax.ShapeDtypeStruct((rows, kv_count * HEAD), jnp.bfloat16),
            jax.ShapeDtypeStruct((rows, kv_count * HEAD), jnp.bfloat16),
            jax.ShapeDtypeStruct((8, HEAD), jnp.float32),
        ),
        in_specs=[pl.BlockSpec(memory_space=pltpu.SMEM)] + [vmem] * 8,
        out_specs=[vmem] * 4,
        scratch_shapes=[
            pltpu.VMEM((cached + rows, HEAD), jnp.bfloat16),
            pltpu.VMEM((cached + rows, 2 * HEAD), jnp.bfloat16),
            pltpu.VMEM((rows, cached + rows), jnp.float32),
            pltpu.VMEM((rows, cached + rows), jnp.float32),
            pltpu.VMEM((rows, HEAD), jnp.float32),
            pltpu.VMEM((rows, HEAD), jnp.float32),
        ],
        compiler_params=pltpu.CompilerParams(vmem_limit_bytes=48 << 20),
        name="attention",
    )(
        length.reshape(1), tok, q_bias.reshape(1, -1), k_bias.reshape(1, -1),
        v_bias.reshape(1, -1), cache_k, cache_v, cosine, sine,
    )


def stats_kernel(n, width, own, out, inbox, send_sems, recv_sems):
    me = lax.axis_index("tp")
    barrier = pltpu.get_barrier_semaphore()
    for step in range(1, n):
        pl.semaphore_signal(barrier, inc=1, device_id={"tp": lax.rem(me + step, n)}, device_id_type=MESH)
    pl.semaphore_wait(barrier, n - 1)
    copies = []
    for step in range(1, n):
        copy = pltpu.make_async_remote_copy(
            src_ref=own, dst_ref=inbox.at[step - 1],
            send_sem=send_sems.at[step - 1], recv_sem=recv_sems.at[step - 1],
            device_id={"tp": lax.rem(me + step, n)}, device_id_type=MESH,
        )
        copy.start()
        copies.append(copy)
    for copy in copies:
        copy.wait()
    squares, top = own[0:1, :], own[1:2, :]
    for step in range(1, n):
        squares = squares + inbox[step - 1, 0:1, :]
        top = jnp.maximum(top, inbox[step - 1, 1:2, :])
    norm = jnp.sqrt(jnp.sum(squares, axis=1, keepdims=True) / width + norm_epsilon)
    top = jnp.max(top, axis=1, keepdims=True)
    out[0:1, :] = jnp.broadcast_to(norm, (1, HEAD))
    out[1:2, :] = jnp.broadcast_to(top, (1, HEAD))


def reduce_stats(stats, width):
    n = lax.axis_size("tp")
    vmem = pl.BlockSpec(memory_space=pltpu.VMEM)
    out = pl.pallas_call(
        functools.partial(stats_kernel, n, width),
        out_shape=jax.ShapeDtypeStruct((8, HEAD), jnp.float32),
        in_specs=[vmem],
        out_specs=vmem,
        scratch_shapes=[
            pltpu.VMEM((n - 1, 8, HEAD), jnp.float32),
            pltpu.SemaphoreType.DMA((n - 1,)),
            pltpu.SemaphoreType.DMA((n - 1,)),
        ],
        compiler_params=pltpu.CompilerParams(collective_id=1, has_side_effects=True),
        name="stats",
    )(stats)
    return out[0, 0:1], out[1, 0:1]


def split_kv(q, k, v):
    kv_count = k.shape[1] // HEAD
    wide = q.shape[1] // kv_count
    return jnp.stack(
        [
            jnp.concatenate(
                [
                    q[:, i * wide : (i + 1) * wide],
                    k[:, i * HEAD : (i + 1) * HEAD],
                    v[:, i * HEAD : (i + 1) * HEAD],
                ],
                axis=1,
            )
            for i in range(kv_count)
        ]
    )


def exchange(tok, deal):
    slots = lax.axis_size("seq")
    slot_ids = jnp.arange(slots, dtype=jnp.int32)
    inverse = jnp.sum(jnp.where(deal[None, :] == slot_ids[:, None], slot_ids[None, :], 0), axis=1)
    flat = tok.reshape(slots, -1, tok.shape[2])
    spread = lax.all_to_all(flat, "seq", split_axis=0, concat_axis=0, tiled=True)
    picked = jnp.take(spread, inverse, axis=0)
    settled = lax.all_to_all(picked, "seq", split_axis=0, concat_axis=0, tiled=True)
    return settled.reshape(tok.shape)


def body(q_new, k_new, v_new, q_bias, k_bias, v_bias, cache_k, cache_v, deal, cache_len):
    rows = q_new.shape[0]
    length = cache_len[lax.axis_index("seq")]
    cosine, sine = tables(length, rows)
    tok = exchange(split_kv(q_new, k_new, v_new), deal)
    attn_out, new_keys, new_values, stats = attend(
        length, tok, q_bias, k_bias, v_bias, cache_k, cache_v, cosine, sine
    )
    last_norm, top_logit = reduce_stats(stats, q_new.shape[1] * lax.axis_size("tp"))
    return attn_out, new_keys, new_values, last_norm, top_logit


def solution(mesh):
    return jax.shard_map(
        body,
        mesh=mesh,
        in_specs=(
            P("seq", "tp"), P("seq", "tp"), P("seq", "tp"), P("tp"), P("tp"), P("tp"),
            P("seq", "tp"), P("seq", "tp"), P(), P(),
        ),
        out_specs=(P("seq", "tp"), P("seq", "tp"), P("seq", "tp"), P("seq"), P("seq")),
        check_vma=False,
    )
```

```python
import functools
import math

import jax
import jax.numpy as jnp
from jax import lax
from jax.experimental import pallas as pl
from jax.experimental.pallas import tpu as pltpu
from jax.sharding import PartitionSpec as P

HEAD = 128
MESH = pl.DeviceIdType.MESH

theta_base = 1000000.0
norm_epsilon = 1e-06
scale = HEAD**-0.5
exp2_scale = scale * math.log2(math.e)
low_score = -3.0e38


def tables(length, rows):
    half_dim = HEAD // 2
    positions = length + jnp.arange(rows, dtype=jnp.int32)
    frequency = theta_base ** (-2.0 * jnp.arange(half_dim, dtype=jnp.float32) / HEAD)
    angles = positions.astype(jnp.float32)[:, None] * frequency[None, :]
    cosine, sine = jnp.cos(angles), jnp.sin(angles)
    return (
        jnp.concatenate([cosine, cosine], axis=1),
        jnp.concatenate([-sine, sine], axis=1),
    )


def rope(x, cosine, sine):
    return x * cosine + pltpu.roll(x, HEAD // 2, 1) * sine


def attention_kernel(
    carried, length_ref, tok, q_bias, k_bias, v_bias, cache_k, cache_v, cosine, sine, *refs
):
    out, new_keys, new_values, stats, keys, values, s_a, s_b, m_a, m_b = refs[carried:]
    rows = tok.shape[1]
    kv_count = tok.shape[0]
    cached = cache_k.shape[0]
    group = tok.shape[2] // HEAD - 2
    half = 256
    halves = rows // half
    length = length_ref[0]

    stats[...] = jnp.zeros_like(stats)
    stats[1:2, :] = jnp.full((1, HEAD), low_score, jnp.float32)
    causal = lax.broadcasted_iota(jnp.int32, (half, half), 1) <= lax.broadcasted_iota(
        jnp.int32, (half, half), 0
    )

    def prepare(kv):
        at = slice(kv * HEAD, (kv + 1) * HEAD)
        valid = lax.broadcasted_iota(jnp.int32, (cached, HEAD), 0) < length
        keys[:cached, :] = jnp.where(valid, cache_k[:, at], cache_k[0:1, at])
        values[:cached, :HEAD] = jnp.where(valid, cache_v[:, at], jnp.bfloat16(0))
        values[:cached, HEAD:] = jnp.where(valid, jnp.bfloat16(1), jnp.bfloat16(0))
        fresh = tok[kv, :, group * HEAD : (group + 1) * HEAD].astype(jnp.float32)
        fresh = fresh + k_bias[0:1, at].astype(jnp.float32)
        fresh = rope(fresh, cosine[...], sine[...]).astype(jnp.bfloat16)
        keys[cached:, :] = fresh
        new_keys[:, at] = fresh
        fresh = tok[kv, :, (group + 1) * HEAD :].astype(jnp.float32)
        fresh = (fresh + v_bias[0:1, at].astype(jnp.float32)).astype(jnp.bfloat16)
        values[cached:, :HEAD] = fresh
        values[cached:, HEAD:] = jnp.ones((rows, HEAD), jnp.bfloat16)
        new_values[:, at] = fresh

    def key_blocks(part):
        blocks = [(first, False) for first in range(0, cached, half)]
        blocks += [(cached + half * i, i == part) for i in range(part + 1)]
        return blocks

    def score(kv, head, s_ref, m_ref):
        at = pl.ds(pl.multiple_of(head * HEAD, HEAD), HEAD)
        bias_at = pl.ds(pl.multiple_of((kv * group + head) * HEAD, HEAD), HEAD)
        bias = q_bias[0:1, bias_at].astype(jnp.float32)
        for part in range(halves):
            here = slice(part * half, (part + 1) * half)
            x = tok[kv, here, at].astype(jnp.float32) + bias
            query = rope(x, cosine[here, :], sine[here, :]).astype(jnp.bfloat16)
            largest = None
            for first, masked in key_blocks(part):
                s = lax.dot_general(
                    query, keys[first : first + half, :],
                    (((1,), (1,)), ((), ())), preferred_element_type=jnp.float32,
                )
                if masked:
                    s = jnp.where(causal, s, low_score)
                s_ref[here, first : first + half] = s
                local = jnp.maximum(s[:, :HEAD], s[:, HEAD:])
                largest = local if largest is None else jnp.maximum(largest, local)
            m_ref[here, :] = jnp.broadcast_to(
                jnp.max(largest, axis=1, keepdims=True), (half, HEAD)
            )

    def mix(kv, head, s_ref, m_ref):
        out_at = pl.ds(pl.multiple_of((kv * group + head) * HEAD, HEAD), HEAD)
        for part in range(halves):
            here = slice(part * half, (part + 1) * half)
            m = m_ref[here, :]
            m2 = jnp.concatenate([m, m], axis=1)
            total = None
            for first, masked in key_blocks(part):
                w = jnp.exp2((s_ref[here, first : first + half] - m2) * exp2_scale)
                term = jnp.dot(
                    w.astype(jnp.bfloat16), values[first : first + half, :],
                    preferred_element_type=jnp.float32,
                )
                total = term if total is None else total + term
            mixture = total[:, :HEAD] / total[:, HEAD:]
            out[here, out_at] = mixture.astype(jnp.bfloat16)
            if part == halves - 1:
                last = mixture[half - 1 : half, :]
                stats[0:1, :] = stats[0:1, :] + last * last
                stats[1:2, :] = jnp.maximum(stats[1:2, :], m[half - 1 : half, :] * scale)

    for kv in range(kv_count):
        prepare(kv)
        score(kv, 0, s_a, m_a)

        @pl.loop(0, group // 2 - 1)
        def _(i):
            score(kv, 2 * i + 1, s_b, m_b)
            mix(kv, 2 * i, s_a, m_a)
            score(kv, 2 * i + 2, s_a, m_a)
            mix(kv, 2 * i + 1, s_b, m_b)

        score(kv, group - 1, s_b, m_b)
        mix(kv, group - 2, s_a, m_a)
        mix(kv, group - 1, s_b, m_b)


def attend(kv, kv_count, carried, length, tok, q_bias, k_bias, v_bias, cache_k, cache_v, cosine, sine):
    _, rows, _ = tok.shape
    cached = cache_k.shape[0]
    wide = q_bias.shape[0] // kv_count
    whole = lambda shape: pl.BlockSpec(shape, lambda i: (0,) * len(shape))
    columns = lambda count, width: pl.BlockSpec((count, width), lambda i: (0, kv))
    out_shape = (
        jax.ShapeDtypeStruct((rows, kv_count * wide), jnp.bfloat16),
        jax.ShapeDtypeStruct((rows, kv_count * HEAD), jnp.bfloat16),
        jax.ShapeDtypeStruct((rows, kv_count * HEAD), jnp.bfloat16),
    )
    operands = 9
    flops = 2 * rows * (cached + rows) * 3 * wide
    return pl.pallas_call(
        functools.partial(attention_kernel, len(carried)),
        grid=(1,),
        out_shape=out_shape + (jax.ShapeDtypeStruct((8, HEAD), jnp.float32),),
        in_specs=[
            pl.BlockSpec(memory_space=pltpu.SMEM),
            whole(tok.shape),
            columns(1, wide), columns(1, HEAD), columns(1, HEAD),
            columns(cached, HEAD), columns(cached, HEAD),
            whole(cosine.shape), whole(sine.shape),
        ] + [pl.BlockSpec(memory_space=pl.ANY)] * len(carried),
        out_specs=[
            columns(rows, wide), columns(rows, HEAD), columns(rows, HEAD), whole((8, HEAD)),
        ],
        scratch_shapes=[
            pltpu.VMEM((cached + rows, HEAD), jnp.bfloat16),
            pltpu.VMEM((cached + rows, 2 * HEAD), jnp.bfloat16),
            pltpu.VMEM((rows, cached + rows), jnp.float32),
            pltpu.VMEM((rows, cached + rows), jnp.float32),
            pltpu.VMEM((rows, HEAD), jnp.float32),
            pltpu.VMEM((rows, HEAD), jnp.float32),
        ],
        input_output_aliases={operands + i: i for i in range(len(carried))},
        compiler_params=pltpu.CompilerParams(vmem_limit_bytes=48 << 20),
        cost_estimate=pl.CostEstimate(
            flops=flops, bytes_accessed=8 << 20, transcendentals=rows * (cached + rows) * (wide // HEAD)
        ),
        name="attention",
    )(
        length.reshape(1), tok, q_bias.reshape(1, -1), k_bias.reshape(1, -1),
        v_bias.reshape(1, -1), cache_k, cache_v, cosine, sine, *carried,
    )


def stats_kernel(n, width, own, out, inbox, send_sems, recv_sems):
    me = lax.axis_index("tp")
    barrier = pltpu.get_barrier_semaphore()
    for step in range(1, n):
        pl.semaphore_signal(barrier, inc=1, device_id={"tp": lax.rem(me + step, n)}, device_id_type=MESH)
    pl.semaphore_wait(barrier, n - 1)
    copies = []
    for step in range(1, n):
        copy = pltpu.make_async_remote_copy(
            src_ref=own, dst_ref=inbox.at[step - 1],
            send_sem=send_sems.at[step - 1], recv_sem=recv_sems.at[step - 1],
            device_id={"tp": lax.rem(me + step, n)}, device_id_type=MESH,
        )
        copy.start()
        copies.append(copy)
    for copy in copies:
        copy.wait()
    squares, top = own[0:1, :], own[1:2, :]
    for step in range(1, n):
        squares = squares + inbox[step - 1, 0:1, :]
        top = jnp.maximum(top, inbox[step - 1, 1:2, :])
    norm = jnp.sqrt(jnp.sum(squares, axis=1, keepdims=True) / width + norm_epsilon)
    top = jnp.max(top, axis=1, keepdims=True)
    out[0:1, :] = jnp.broadcast_to(norm, (1, HEAD))
    out[1:2, :] = jnp.broadcast_to(top, (1, HEAD))


def reduce_stats(parts, width):
    n = lax.axis_size("tp")
    stats = jnp.concatenate(
        [
            functools.reduce(jnp.add, [part[0:1] for part in parts]),
            functools.reduce(jnp.maximum, [part[1:] for part in parts]),
        ]
    )
    vmem = pl.BlockSpec(memory_space=pltpu.VMEM)
    out = pl.pallas_call(
        functools.partial(stats_kernel, n, width),
        out_shape=jax.ShapeDtypeStruct((8, HEAD), jnp.float32),
        in_specs=[vmem],
        out_specs=vmem,
        scratch_shapes=[
            pltpu.VMEM((n - 1, 8, HEAD), jnp.float32),
            pltpu.SemaphoreType.DMA((n - 1,)),
            pltpu.SemaphoreType.DMA((n - 1,)),
        ],
        compiler_params=pltpu.CompilerParams(collective_id=1, has_side_effects=True),
        name="stats",
    )(stats)
    return out[0, 0:1], out[1, 0:1]


def packet(kv, q, k, v):
    wide = q.shape[1] // (k.shape[1] // HEAD)
    at = slice(kv * HEAD, (kv + 1) * HEAD)
    return jnp.concatenate([q[:, kv * wide : (kv + 1) * wide], k[:, at], v[:, at]], axis=1)


def spread(tok):
    slots = lax.axis_size("seq")
    flat = tok.reshape(slots, -1, tok.shape[1])
    return lax.all_to_all(flat, "seq", split_axis=0, concat_axis=0, tiled=True)


def settle(scattered, inverse):
    picked = jnp.take(scattered, inverse, axis=0, mode="clip")
    settled = lax.all_to_all(picked, "seq", split_axis=0, concat_axis=0, tiled=True)
    return settled.reshape(1, -1, scattered.shape[2])


def body(q_new, k_new, v_new, q_bias, k_bias, v_bias, cache_k, cache_v, deal, cache_len):
    rows = q_new.shape[0]
    kv_count = k_new.shape[1] // HEAD
    length = cache_len[lax.axis_index("seq")]
    cosine, sine = tables(length, rows)
    slot_ids = jnp.arange(lax.axis_size("seq"), dtype=jnp.int32)
    inverse = jnp.sum(jnp.where(deal[None, :] == slot_ids[:, None], slot_ids[None, :], 0), axis=1)
    scattered = [spread(packet(kv, q_new, k_new, v_new)) for kv in range(kv_count)]
    arrived = [settle(part, inverse) for part in scattered]
    carried, parts = (), []
    for kv in range(kv_count):
        *carried, part = attend(
            kv, kv_count, carried, length, arrived[kv], q_bias, k_bias, v_bias,
            cache_k, cache_v, cosine, sine,
        )
        parts.append(part)
    attn_out, new_keys, new_values = carried
    last_norm, top_logit = reduce_stats(parts, q_new.shape[1] * lax.axis_size("tp"))
    return attn_out, new_keys, new_values, last_norm, top_logit


def solution(mesh):
    return jax.shard_map(
        body,
        mesh=mesh,
        in_specs=(
            P("seq", "tp"), P("seq", "tp"), P("seq", "tp"), P("tp"), P("tp"), P("tp"),
            P("seq", "tp"), P("seq", "tp"), P(), P(),
        ),
        out_specs=(P("seq", "tp"), P("seq", "tp"), P("seq", "tp"), P("seq"), P("seq")),
        check_vma=False,
    )
```

```python
import functools
import math

import jax
import jax.numpy as jnp
from jax import lax
from jax.experimental import pallas as pl
from jax.experimental.pallas import tpu as pltpu
from jax.sharding import PartitionSpec as P

HEAD = 128
MESH = pl.DeviceIdType.MESH

theta_base = 1000000.0
norm_epsilon = 1e-06
scale = HEAD**-0.5
exp2_scale = scale * math.log2(math.e)
low_score = -3.0e38


def tables(length, rows):
    half_dim = HEAD // 2
    positions = length + jnp.arange(rows, dtype=jnp.int32)
    frequency = theta_base ** (-2.0 * jnp.arange(half_dim, dtype=jnp.float32) / HEAD)
    angles = positions.astype(jnp.float32)[:, None] * frequency[None, :]
    cosine, sine = jnp.cos(angles), jnp.sin(angles)
    return (
        jnp.concatenate([cosine, cosine], axis=1),
        jnp.concatenate([-sine, sine], axis=1),
    )


def rope(x, cosine, sine):
    return x * cosine + pltpu.roll(x, HEAD // 2, 1) * sine


def packet_columns(q_width, k_width):
    half = q_width // 2
    return 0, half, half + k_width, half + 2 * k_width


def attention_kernel(
    length_ref, tok, q_bias, k_bias, v_bias, cache_k, cache_v, cosine, sine,
    out, new_keys, new_values, stats,
    keys, values, s_a, s_b, m_a, m_b,
):
    pieces, tall, _ = tok.shape
    rows = pieces * tall
    kv_count = k_bias.shape[1] // HEAD
    cached = cache_k.shape[0]
    group = q_bias.shape[1] // HEAD // kv_count
    _, k_at, v_at, _ = packet_columns(q_bias.shape[1], k_bias.shape[1])
    half = 256
    halves = rows // half
    length = length_ref[0]

    stats[...] = jnp.zeros_like(stats)
    stats[1:2, :] = jnp.full((1, HEAD), low_score, jnp.float32)
    causal = lax.broadcasted_iota(jnp.int32, (half, half), 1) <= lax.broadcasted_iota(
        jnp.int32, (half, half), 0
    )

    def arrived(first, count, at):
        x = tok[first // tall : (first + count) // tall, :, at].astype(jnp.float32)
        return x.reshape(count, HEAD)

    def prepare(kv):
        at = slice(kv * HEAD, (kv + 1) * HEAD)
        valid = lax.broadcasted_iota(jnp.int32, (cached, HEAD), 0) < length
        keys[:cached, :] = jnp.where(valid, cache_k[:, at], cache_k[0:1, at])
        values[:cached, :HEAD] = jnp.where(valid, cache_v[:, at], jnp.bfloat16(0))
        values[:cached, HEAD:] = jnp.where(valid, jnp.bfloat16(1), jnp.bfloat16(0))
        fresh = arrived(0, rows, slice(k_at + kv * HEAD, k_at + (kv + 1) * HEAD))
        fresh = fresh + k_bias[0:1, at].astype(jnp.float32)
        fresh = rope(fresh, cosine[...], sine[...]).astype(jnp.bfloat16)
        keys[cached:, :] = fresh
        new_keys[:, at] = fresh
        fresh = arrived(0, rows, slice(v_at + kv * HEAD, v_at + (kv + 1) * HEAD))
        fresh = (fresh + v_bias[0:1, at].astype(jnp.float32)).astype(jnp.bfloat16)
        values[cached:, :HEAD] = fresh
        values[cached:, HEAD:] = jnp.ones((rows, HEAD), jnp.bfloat16)
        new_values[:, at] = fresh

    def key_blocks(part):
        blocks = [(first, False) for first in range(0, cached, half)]
        blocks += [(cached + half * i, i == part) for i in range(part + 1)]
        return blocks

    def score(kv, head, s_ref, m_ref):
        q_at = packet_columns(q_bias.shape[1], k_bias.shape[1])[0 if kv == 0 else 3]
        at = pl.ds(pl.multiple_of(q_at + head * HEAD, HEAD), HEAD)
        bias_at = pl.ds(pl.multiple_of((kv * group + head) * HEAD, HEAD), HEAD)
        bias = q_bias[0:1, bias_at].astype(jnp.float32)
        for part in range(halves):
            here = slice(part * half, (part + 1) * half)
            x = arrived(part * half, half, at) + bias
            query = rope(x, cosine[here, :], sine[here, :]).astype(jnp.bfloat16)
            largest = None
            for first, masked in key_blocks(part):
                s = lax.dot_general(
                    query, keys[first : first + half, :],
                    (((1,), (1,)), ((), ())), preferred_element_type=jnp.float32,
                )
                if masked:
                    s = jnp.where(causal, s, low_score)
                s_ref[here, first : first + half] = s
                local = jnp.maximum(s[:, :HEAD], s[:, HEAD:])
                largest = local if largest is None else jnp.maximum(largest, local)
            m_ref[here, :] = jnp.broadcast_to(
                jnp.max(largest, axis=1, keepdims=True), (half, HEAD)
            )

    def mix(kv, head, s_ref, m_ref):
        out_at = pl.ds(pl.multiple_of((kv * group + head) * HEAD, HEAD), HEAD)
        for part in range(halves):
            here = slice(part * half, (part + 1) * half)
            m = m_ref[here, :]
            m2 = jnp.concatenate([m, m], axis=1)
            total = None
            for first, masked in key_blocks(part):
                w = jnp.exp2((s_ref[here, first : first + half] - m2) * exp2_scale)
                term = jnp.dot(
                    w.astype(jnp.bfloat16), values[first : first + half, :],
                    preferred_element_type=jnp.float32,
                )
                total = term if total is None else total + term
            mixture = total[:, :HEAD] / total[:, HEAD:]
            out[here, out_at] = mixture.astype(jnp.bfloat16)
            if part == halves - 1:
                last = mixture[half - 1 : half, :]
                stats[0:1, :] = stats[0:1, :] + last * last
                stats[1:2, :] = jnp.maximum(stats[1:2, :], m[half - 1 : half, :] * scale)

    for kv in range(kv_count):
        prepare(kv)
        score(kv, 0, s_a, m_a)

        @pl.loop(0, group // 2 - 1)
        def _(i):
            score(kv, 2 * i + 1, s_b, m_b)
            mix(kv, 2 * i, s_a, m_a)
            score(kv, 2 * i + 2, s_a, m_a)
            mix(kv, 2 * i + 1, s_b, m_b)

        score(kv, group - 1, s_b, m_b)
        mix(kv, group - 2, s_a, m_a)
        mix(kv, group - 1, s_b, m_b)


def attend(length, tok, q_bias, k_bias, v_bias, cache_k, cache_v, cosine, sine):
    rows = tok.shape[0] * tok.shape[1]
    kv_count = k_bias.shape[0] // HEAD
    cached = cache_k.shape[0]
    vmem = pl.BlockSpec(memory_space=pltpu.VMEM)
    return pl.pallas_call(
        attention_kernel,
        out_shape=(
            jax.ShapeDtypeStruct((rows, q_bias.shape[0]), jnp.bfloat16),
            jax.ShapeDtypeStruct((rows, kv_count * HEAD), jnp.bfloat16),
            jax.ShapeDtypeStruct((rows, kv_count * HEAD), jnp.bfloat16),
            jax.ShapeDtypeStruct((8, HEAD), jnp.float32),
        ),
        in_specs=[pl.BlockSpec(memory_space=pltpu.SMEM)] + [vmem] * 8,
        out_specs=[vmem] * 4,
        scratch_shapes=[
            pltpu.VMEM((cached + rows, HEAD), jnp.bfloat16),
            pltpu.VMEM((cached + rows, 2 * HEAD), jnp.bfloat16),
            pltpu.VMEM((rows, cached + rows), jnp.float32),
            pltpu.VMEM((rows, cached + rows), jnp.float32),
            pltpu.VMEM((rows, HEAD), jnp.float32),
            pltpu.VMEM((rows, HEAD), jnp.float32),
        ],
        compiler_params=pltpu.CompilerParams(vmem_limit_bytes=48 << 20),
        name="attention",
    )(
        length.reshape(1), tok, q_bias.reshape(1, -1), k_bias.reshape(1, -1),
        v_bias.reshape(1, -1), cache_k, cache_v, cosine, sine,
    )


def stats_kernel(n, width, own, out, inbox, send_sems, recv_sems):
    me = lax.axis_index("tp")
    barrier = pltpu.get_barrier_semaphore()
    for step in range(1, n):
        pl.semaphore_signal(barrier, inc=1, device_id={"tp": lax.rem(me + step, n)}, device_id_type=MESH)
    pl.semaphore_wait(barrier, n - 1)
    copies = []
    for step in range(1, n):
        copy = pltpu.make_async_remote_copy(
            src_ref=own, dst_ref=inbox.at[step - 1],
            send_sem=send_sems.at[step - 1], recv_sem=recv_sems.at[step - 1],
            device_id={"tp": lax.rem(me + step, n)}, device_id_type=MESH,
        )
        copy.start()
        copies.append(copy)
    for copy in copies:
        copy.wait()
    squares, top = own[0:1, :], own[1:2, :]
    for step in range(1, n):
        squares = squares + inbox[step - 1, 0:1, :]
        top = jnp.maximum(top, inbox[step - 1, 1:2, :])
    norm = jnp.sqrt(jnp.sum(squares, axis=1, keepdims=True) / width + norm_epsilon)
    top = jnp.max(top, axis=1, keepdims=True)
    out[0:1, :] = jnp.broadcast_to(norm, (1, HEAD))
    out[1:2, :] = jnp.broadcast_to(top, (1, HEAD))


def reduce_stats(stats, width):
    n = lax.axis_size("tp")
    vmem = pl.BlockSpec(memory_space=pltpu.VMEM)
    out = pl.pallas_call(
        functools.partial(stats_kernel, n, width),
        out_shape=jax.ShapeDtypeStruct((8, HEAD), jnp.float32),
        in_specs=[vmem],
        out_specs=vmem,
        scratch_shapes=[
            pltpu.VMEM((n - 1, 8, HEAD), jnp.float32),
            pltpu.SemaphoreType.DMA((n - 1,)),
            pltpu.SemaphoreType.DMA((n - 1,)),
        ],
        compiler_params=pltpu.CompilerParams(collective_id=1, has_side_effects=True),
        name="stats",
    )(stats)
    return out[0, 0:1], out[1, 0:1]


def exchange_kernel(n, parts, *refs):
    *sources, out, send_sem, recv_sem, own_sems = refs
    me = lax.axis_index("seq")
    barrier = pltpu.get_barrier_semaphore()

    def greet(step, carry):
        pl.semaphore_signal(barrier, inc=1, device_id={"seq": lax.rem(me + step, n)}, device_id_type=MESH)
        return carry

    lax.fori_loop(1, n, greet, 0)
    pl.semaphore_wait(barrier, n - 1)

    def send(peer):
        for source, first, width, to in parts:
            pltpu.make_async_remote_copy(
                src_ref=sources[source].at[peer, :, first : first + width],
                dst_ref=out.at[me, :, to : to + width],
                send_sem=send_sem, recv_sem=recv_sem,
                device_id={"seq": peer}, device_id_type=MESH,
            ).start()

    def send_both_ways(step, carry):
        send(lax.rem(me + step, n))
        send(lax.rem(me + n - step, n))
        return carry

    lax.fori_loop(1, n // 2, send_both_ways, 0)
    send(lax.rem(me + n // 2, n))
    own = [
        pltpu.make_async_copy(
            sources[source].at[me, :, first : first + width],
            out.at[me, :, to : to + width], own_sems.at[i],
        )
        for i, (source, first, width, to) in enumerate(parts)
    ]
    for copy in own:
        copy.start()
    for copy in own:
        copy.wait()
    others = out.at[pl.ds(0, n - 1)]
    pltpu.make_async_copy(others, others, recv_sem).wait()
    pltpu.make_async_copy(others, others, send_sem).wait()


def exchange(parts, width, collective_id, *sources):
    n = lax.axis_size("seq")
    anywhere = pl.BlockSpec(memory_space=pl.ANY)
    return pl.pallas_call(
        functools.partial(exchange_kernel, n, parts),
        out_shape=jax.ShapeDtypeStruct((n, sources[0].shape[1], width), jnp.bfloat16),
        in_specs=[anywhere] * len(sources),
        out_specs=anywhere,
        scratch_shapes=[
            pltpu.SemaphoreType.DMA, pltpu.SemaphoreType.DMA,
            pltpu.SemaphoreType.DMA((len(parts),)),
        ],
        compiler_params=pltpu.CompilerParams(collective_id=collective_id, has_side_effects=True),
        name="exchange",
    )(*sources)


def deliver(q, k, v, deal):
    slots = lax.axis_size("seq")
    slot_ids = jnp.arange(slots, dtype=jnp.int32)
    inverse = jnp.sum(jnp.where(deal[None, :] == slot_ids[:, None], slot_ids[None, :], 0), axis=1)
    half, k_width = q.shape[1] // 2, k.shape[1]
    width = q.shape[1] + 2 * k_width
    first_at, k_at, v_at, second_at = packet_columns(q.shape[1], k_width)
    q, k, v = (x.reshape(slots, -1, x.shape[1]) for x in (q, k, v))
    parts = ((0, 0, half, first_at), (1, 0, k_width, k_at), (2, 0, k_width, v_at), (0, half, half, second_at))
    spread = exchange(parts, width, 2, q, k, v)
    picked = jnp.take(spread, inverse, axis=0, mode="clip")
    return exchange(((0, 0, width, 0),), width, 3, picked)


def body(q_new, k_new, v_new, q_bias, k_bias, v_bias, cache_k, cache_v, deal, cache_len):
    rows = q_new.shape[0]
    length = cache_len[lax.axis_index("seq")]
    cosine, sine = tables(length, rows)
    tok = deliver(q_new, k_new, v_new, deal)
    attn_out, new_keys, new_values, stats = attend(
        length, tok, q_bias, k_bias, v_bias, cache_k, cache_v, cosine, sine
    )
    last_norm, top_logit = reduce_stats(stats, q_new.shape[1] * lax.axis_size("tp"))
    return attn_out, new_keys, new_values, last_norm, top_logit


def solution(mesh):
    return jax.shard_map(
        body,
        mesh=mesh,
        in_specs=(
            P("seq", "tp"), P("seq", "tp"), P("seq", "tp"), P("tp"), P("tp"), P("tp"),
            P("seq", "tp"), P("seq", "tp"), P(), P(),
        ),
        out_specs=(P("seq", "tp"), P("seq", "tp"), P("seq", "tp"), P("seq"), P("seq")),
        check_vma=False,
    )
```

```python
import functools
import math

import jax
import jax.numpy as jnp
from jax import lax
from jax.experimental import pallas as pl
from jax.experimental.pallas import tpu as pltpu
from jax.sharding import PartitionSpec as P

HEAD = 128
MESH = pl.DeviceIdType.MESH

theta_base = 1000000.0
norm_epsilon = 1e-06
scale = HEAD**-0.5
exp2_scale = scale * math.log2(math.e)
low_score = -3.0e38


def tables(length, rows):
    half_dim = HEAD // 2
    positions = length + jnp.arange(rows, dtype=jnp.int32)
    frequency = theta_base ** (-2.0 * jnp.arange(half_dim, dtype=jnp.float32) / HEAD)
    angles = positions.astype(jnp.float32)[:, None] * frequency[None, :]
    cosine, sine = jnp.cos(angles), jnp.sin(angles)
    return (
        jnp.concatenate([cosine, cosine], axis=1),
        jnp.concatenate([-sine, sine], axis=1),
    )


def rope(x, cosine, sine):
    return x * cosine + pltpu.roll(x, HEAD // 2, 1) * sine


def packet_columns(q_width, k_width):
    half = q_width // 2
    return 0, half, half + k_width, half + 2 * k_width


def greet_all(n):
    me = lax.axis_index("seq")
    barrier = pltpu.get_barrier_semaphore()

    def greet(step, carry):
        pl.semaphore_signal(barrier, inc=1, device_id={"seq": lax.rem(me + step, n)}, device_id_type=MESH)
        return carry

    lax.fori_loop(1, n, greet, 0)
    pl.semaphore_wait(barrier, n - 1)
    return me


def send_all(n, me, parts, out, send_sem, recv_sem):
    def send(peer):
        for source, first, width, to in parts:
            pltpu.make_async_remote_copy(
                src_ref=source.at[peer, :, first : first + width],
                dst_ref=out.at[me, :, to : to + width],
                send_sem=send_sem, recv_sem=recv_sem,
                device_id={"seq": peer}, device_id_type=MESH,
            ).start()

    def send_both_ways(step, carry):
        send(lax.rem(me + step, n))
        send(lax.rem(me + n - step, n))
        return carry

    lax.fori_loop(1, n // 2, send_both_ways, 0)
    send(lax.rem(me + n // 2, n))


def attention_kernel(
    n, length_ref, picked, q_bias, k_bias, v_bias, cache_k, cache_v, cosine, sine,
    out, new_keys, new_values, stats,
    tok, keys, values, s_a, s_b, m_a, m_b, send_sems, recv_sems, own_sems,
):
    pieces, tall, width = tok.shape
    rows = pieces * tall
    me = greet_all(n)
    kv_count = k_bias.shape[1] // HEAD
    cached = cache_k.shape[0]
    group = q_bias.shape[1] // HEAD // kv_count
    _, k_at, v_at, _ = packet_columns(q_bias.shape[1], k_bias.shape[1])
    half = 256
    halves = rows // half
    length = length_ref[0]

    first_chunk = packet_columns(q_bias.shape[1], k_bias.shape[1])[3]
    chunks = (slice(0, first_chunk), slice(first_chunk, width))
    for i, at in enumerate(chunks):
        send_all(
            n, me, [(picked, at.start, at.stop - at.start, at.start)], tok,
            send_sems.at[i], recv_sems.at[i],
        )
    own = [
        pltpu.make_async_copy(picked.at[me, :, at], tok.at[me, :, at], own_sems.at[i])
        for i, at in enumerate(chunks)
    ]
    for copy in own:
        copy.start()

    def wait_for(i, sems):
        others = tok.at[pl.ds(0, n - 1), :, chunks[i]]
        pltpu.make_async_copy(others, others, sems.at[i]).wait()

    stats[...] = jnp.zeros_like(stats)
    stats[1:2, :] = jnp.full((1, HEAD), low_score, jnp.float32)
    causal = lax.broadcasted_iota(jnp.int32, (half, half), 1) <= lax.broadcasted_iota(
        jnp.int32, (half, half), 0
    )

    def arrived(first, count, at):
        x = tok[first // tall : (first + count) // tall, :, at].astype(jnp.float32)
        return x.reshape(count, HEAD)

    def prepare_cached(kv):
        at = slice(kv * HEAD, (kv + 1) * HEAD)
        valid = lax.broadcasted_iota(jnp.int32, (cached, HEAD), 0) < length
        keys[:cached, :] = jnp.where(valid, cache_k[:, at], cache_k[0:1, at])
        values[:cached, :HEAD] = jnp.where(valid, cache_v[:, at], jnp.bfloat16(0))
        values[:cached, HEAD:] = jnp.where(valid, jnp.bfloat16(1), jnp.bfloat16(0))

    def prepare_new(kv):
        at = slice(kv * HEAD, (kv + 1) * HEAD)
        fresh = arrived(0, rows, slice(k_at + kv * HEAD, k_at + (kv + 1) * HEAD))
        fresh = fresh + k_bias[0:1, at].astype(jnp.float32)
        fresh = rope(fresh, cosine[...], sine[...]).astype(jnp.bfloat16)
        keys[cached:, :] = fresh
        new_keys[:, at] = fresh
        fresh = arrived(0, rows, slice(v_at + kv * HEAD, v_at + (kv + 1) * HEAD))
        fresh = (fresh + v_bias[0:1, at].astype(jnp.float32)).astype(jnp.bfloat16)
        values[cached:, :HEAD] = fresh
        values[cached:, HEAD:] = jnp.ones((rows, HEAD), jnp.bfloat16)
        new_values[:, at] = fresh

    def key_blocks(part):
        blocks = [(first, False) for first in range(0, cached, half)]
        blocks += [(cached + half * i, i == part) for i in range(part + 1)]
        return blocks

    def score(kv, head, s_ref, m_ref):
        q_at = packet_columns(q_bias.shape[1], k_bias.shape[1])[0 if kv == 0 else 3]
        at = pl.ds(pl.multiple_of(q_at + head * HEAD, HEAD), HEAD)
        bias_at = pl.ds(pl.multiple_of((kv * group + head) * HEAD, HEAD), HEAD)
        bias = q_bias[0:1, bias_at].astype(jnp.float32)
        for part in range(halves):
            here = slice(part * half, (part + 1) * half)
            x = arrived(part * half, half, at) + bias
            query = rope(x, cosine[here, :], sine[here, :]).astype(jnp.bfloat16)
            largest = None
            for first, masked in key_blocks(part):
                s = lax.dot_general(
                    query, keys[first : first + half, :],
                    (((1,), (1,)), ((), ())), preferred_element_type=jnp.float32,
                )
                if masked:
                    s = jnp.where(causal, s, low_score)
                s_ref[here, first : first + half] = s
                local = jnp.maximum(s[:, :HEAD], s[:, HEAD:])
                largest = local if largest is None else jnp.maximum(largest, local)
            m_ref[here, :] = jnp.broadcast_to(
                jnp.max(largest, axis=1, keepdims=True), (half, HEAD)
            )

    def mix(kv, head, s_ref, m_ref):
        out_at = pl.ds(pl.multiple_of((kv * group + head) * HEAD, HEAD), HEAD)
        for part in range(halves):
            here = slice(part * half, (part + 1) * half)
            m = m_ref[here, :]
            m2 = jnp.concatenate([m, m], axis=1)
            total = None
            for first, masked in key_blocks(part):
                w = jnp.exp2((s_ref[here, first : first + half] - m2) * exp2_scale)
                term = jnp.dot(
                    w.astype(jnp.bfloat16), values[first : first + half, :],
                    preferred_element_type=jnp.float32,
                )
                total = term if total is None else total + term
            mixture = total[:, :HEAD] / total[:, HEAD:]
            out[here, out_at] = mixture.astype(jnp.bfloat16)
            if part == halves - 1:
                last = mixture[half - 1 : half, :]
                stats[0:1, :] = stats[0:1, :] + last * last
                stats[1:2, :] = jnp.maximum(stats[1:2, :], m[half - 1 : half, :] * scale)

    for kv in range(kv_count):
        prepare_cached(kv)
        own[kv].wait()
        wait_for(kv, recv_sems)
        prepare_new(kv)
        score(kv, 0, s_a, m_a)

        @pl.loop(0, group // 2 - 1)
        def _(i):
            score(kv, 2 * i + 1, s_b, m_b)
            mix(kv, 2 * i, s_a, m_a)
            score(kv, 2 * i + 2, s_a, m_a)
            mix(kv, 2 * i + 1, s_b, m_b)

        score(kv, group - 1, s_b, m_b)
        mix(kv, group - 2, s_a, m_a)
        mix(kv, group - 1, s_b, m_b)
    for i in range(len(chunks)):
        wait_for(i, send_sems)


def attend(length, picked, q_bias, k_bias, v_bias, cache_k, cache_v, cosine, sine):
    rows = picked.shape[0] * picked.shape[1]
    kv_count = k_bias.shape[0] // HEAD
    cached = cache_k.shape[0]
    vmem = pl.BlockSpec(memory_space=pltpu.VMEM)
    return pl.pallas_call(
        functools.partial(attention_kernel, picked.shape[0]),
        out_shape=(
            jax.ShapeDtypeStruct((rows, q_bias.shape[0]), jnp.bfloat16),
            jax.ShapeDtypeStruct((rows, kv_count * HEAD), jnp.bfloat16),
            jax.ShapeDtypeStruct((rows, kv_count * HEAD), jnp.bfloat16),
            jax.ShapeDtypeStruct((8, HEAD), jnp.float32),
        ),
        in_specs=[pl.BlockSpec(memory_space=pltpu.SMEM), pl.BlockSpec(memory_space=pl.ANY)] + [vmem] * 7,
        out_specs=[vmem] * 4,
        scratch_shapes=[
            pltpu.VMEM(picked.shape, jnp.bfloat16),
            pltpu.VMEM((cached + rows, HEAD), jnp.bfloat16),
            pltpu.VMEM((cached + rows, 2 * HEAD), jnp.bfloat16),
            pltpu.VMEM((rows, cached + rows), jnp.float32),
            pltpu.VMEM((rows, cached + rows), jnp.float32),
            pltpu.VMEM((rows, HEAD), jnp.float32),
            pltpu.VMEM((rows, HEAD), jnp.float32),
            pltpu.SemaphoreType.DMA((2,)),
            pltpu.SemaphoreType.DMA((2,)),
            pltpu.SemaphoreType.DMA((2,)),
        ],
        compiler_params=pltpu.CompilerParams(
            vmem_limit_bytes=48 << 20, collective_id=3, has_side_effects=True
        ),
        name="attention",
    )(
        length.reshape(1), picked, q_bias.reshape(1, -1), k_bias.reshape(1, -1),
        v_bias.reshape(1, -1), cache_k, cache_v, cosine, sine,
    )


def stats_kernel(n, width, own, out, inbox, send_sems, recv_sems):
    me = lax.axis_index("tp")
    barrier = pltpu.get_barrier_semaphore()
    for step in range(1, n):
        pl.semaphore_signal(barrier, inc=1, device_id={"tp": lax.rem(me + step, n)}, device_id_type=MESH)
    pl.semaphore_wait(barrier, n - 1)
    copies = []
    for step in range(1, n):
        copy = pltpu.make_async_remote_copy(
            src_ref=own, dst_ref=inbox.at[step - 1],
            send_sem=send_sems.at[step - 1], recv_sem=recv_sems.at[step - 1],
            device_id={"tp": lax.rem(me + step, n)}, device_id_type=MESH,
        )
        copy.start()
        copies.append(copy)
    for copy in copies:
        copy.wait()
    squares, top = own[0:1, :], own[1:2, :]
    for step in range(1, n):
        squares = squares + inbox[step - 1, 0:1, :]
        top = jnp.maximum(top, inbox[step - 1, 1:2, :])
    norm = jnp.sqrt(jnp.sum(squares, axis=1, keepdims=True) / width + norm_epsilon)
    top = jnp.max(top, axis=1, keepdims=True)
    out[0:1, :] = jnp.broadcast_to(norm, (1, HEAD))
    out[1:2, :] = jnp.broadcast_to(top, (1, HEAD))


def reduce_stats(stats, width):
    n = lax.axis_size("tp")
    vmem = pl.BlockSpec(memory_space=pltpu.VMEM)
    out = pl.pallas_call(
        functools.partial(stats_kernel, n, width),
        out_shape=jax.ShapeDtypeStruct((8, HEAD), jnp.float32),
        in_specs=[vmem],
        out_specs=vmem,
        scratch_shapes=[
            pltpu.VMEM((n - 1, 8, HEAD), jnp.float32),
            pltpu.SemaphoreType.DMA((n - 1,)),
            pltpu.SemaphoreType.DMA((n - 1,)),
        ],
        compiler_params=pltpu.CompilerParams(collective_id=1, has_side_effects=True),
        name="stats",
    )(stats)
    return out[0, 0:1], out[1, 0:1]


def exchange_kernel(n, parts, *refs):
    *sources, out, send_sem, recv_sem, own_sems = refs
    me = greet_all(n)
    send_all(n, me, [(sources[source], *rest) for source, *rest in parts], out, send_sem, recv_sem)
    own = [
        pltpu.make_async_copy(
            sources[source].at[me, :, first : first + width],
            out.at[me, :, to : to + width], own_sems.at[i],
        )
        for i, (source, first, width, to) in enumerate(parts)
    ]
    for copy in own:
        copy.start()
    for copy in own:
        copy.wait()
    others = out.at[pl.ds(0, n - 1)]
    pltpu.make_async_copy(others, others, recv_sem).wait()
    pltpu.make_async_copy(others, others, send_sem).wait()


def exchange(parts, width, collective_id, *sources):
    n = lax.axis_size("seq")
    anywhere = pl.BlockSpec(memory_space=pl.ANY)
    return pl.pallas_call(
        functools.partial(exchange_kernel, n, parts),
        out_shape=jax.ShapeDtypeStruct((n, sources[0].shape[1], width), jnp.bfloat16),
        in_specs=[anywhere] * len(sources),
        out_specs=anywhere,
        scratch_shapes=[
            pltpu.SemaphoreType.DMA, pltpu.SemaphoreType.DMA,
            pltpu.SemaphoreType.DMA((len(parts),)),
        ],
        compiler_params=pltpu.CompilerParams(collective_id=collective_id, has_side_effects=True),
        name="exchange",
    )(*sources)


def spread_pieces(q, k, v, deal):
    slots = lax.axis_size("seq")
    slot_ids = jnp.arange(slots, dtype=jnp.int32)
    inverse = jnp.sum(jnp.where(deal[None, :] == slot_ids[:, None], slot_ids[None, :], 0), axis=1)
    half, k_width = q.shape[1] // 2, k.shape[1]
    width = q.shape[1] + 2 * k_width
    first_at, k_at, v_at, second_at = packet_columns(q.shape[1], k_width)
    q, k, v = (x.reshape(slots, -1, x.shape[1]) for x in (q, k, v))
    parts = ((0, 0, half, first_at), (1, 0, k_width, k_at), (2, 0, k_width, v_at), (0, half, half, second_at))
    spread = exchange(parts, width, 2, q, k, v)
    return jnp.take(spread, inverse, axis=0, mode="clip")


def body(q_new, k_new, v_new, q_bias, k_bias, v_bias, cache_k, cache_v, deal, cache_len):
    rows = q_new.shape[0]
    length = cache_len[lax.axis_index("seq")]
    cosine, sine = tables(length, rows)
    picked = spread_pieces(q_new, k_new, v_new, deal)
    attn_out, new_keys, new_values, stats = attend(
        length, picked, q_bias, k_bias, v_bias, cache_k, cache_v, cosine, sine
    )
    last_norm, top_logit = reduce_stats(stats, q_new.shape[1] * lax.axis_size("tp"))
    return attn_out, new_keys, new_values, last_norm, top_logit


def solution(mesh):
    return jax.shard_map(
        body,
        mesh=mesh,
        in_specs=(
            P("seq", "tp"), P("seq", "tp"), P("seq", "tp"), P("tp"), P("tp"), P("tp"),
            P("seq", "tp"), P("seq", "tp"), P(), P(),
        ),
        out_specs=(P("seq", "tp"), P("seq", "tp"), P("seq", "tp"), P("seq"), P("seq")),
        check_vma=False,
    )
```
